256 devices in a mesh: row: 16 (over z, core), col: 16 (over y, x).
Axes of the slice: x: 4, y: 4, z: 8, core: 2. Of those that a mesh axis runs over, the one named last changes fastest.
Arguments:
- blocks: bfloat16 [16, 16, 5, 128, 8192], P('row', 'col'), may hold values from -6 to 6
- coords: int32 [16, 16, 5, 3], P('row', 'col'), may hold values from 0 to 15, as said below
- counts: int32 [16, 16], P('row', 'col'), may hold values from 1 to 5, as said below
- doc_factor: bfloat16 [32768, 128], P(('col', 'row')), may hold values from -6 to 6
- ctx_factor: bfloat16 [512, 128], P('col'), may hold values from -0.0625 to 0.0625
Outputs:
- mttkrp: float32 [32768, 128], P(('row', 'col'))
The draws below stay inside these ranges and needn't reach their ends.
Inputs may be any that keep to these rules, and one draw needn't show every extreme that they name: coords[..., 0] lies in 0 to 15, coords[..., 1] in 0 to 15, coords[..., 2] in 0 to 7; slots at or past the device's count are ignored. `counts`: some device uses all 5 slots.
All inputs are finite; a program needn't handle non-finite values.
Results may differ from the reference program's by a relative error of at most 0.0029.
Values may be sent and summed in bfloat16 or wider, within the bound.
No kernel may reach another device: no remote copies, remote signals or barrier semaphores. Data moves between devices by JAX's collectives and lax.ppermute only.
A program may use at most 64 MiB of HBM per device.

```python
import jax
import jax.numpy as jnp
from jax import lax

R = 128
BQ = 128
BD = 128
BK = 64
KB = 8
NB_DEV = 5
QBC = 1
DBC = 1
RGROUPS = 16
CGROUPS = 16
QB_ROW = 16
DB_COL = 16
QUERIES = 32768
DOCS = 32768
CTX = 512


def draw_coords(key, part):
    keys = jax.random.split(key, 3)
    shape = (RGROUPS, CGROUPS, NB_DEV)
    query_ids = jax.random.randint(keys[0], shape, 0, QBC * CGROUPS)
    doc_ids = jax.random.randint(keys[1], shape, 0, DBC * RGROUPS)
    ctx_ids = jax.random.randint(keys[2], shape, 0, KB)
    return jnp.stack([query_ids, doc_ids, ctx_ids], axis=-1).astype(jnp.int32)


def draw_counts(key, part):
    keys = jax.random.split(key, 3)
    shape = (RGROUPS, CGROUPS)
    light = jax.random.randint(keys[0], shape, 1, 3)
    heavy = jax.random.randint(keys[1], shape, 0, 4) == 0
    values = jnp.where(heavy, NB_DEV, light).reshape(-1)
    chosen = jax.random.randint(keys[2], (), 0, RGROUPS * CGROUPS)
    values = values.at[chosen].set(NB_DEV)
    return values.reshape(shape).astype(jnp.int32)


def levels(key, shape, pieces, smallest, top_value):
    gain, own = 1.0, jax.random.fold_in(key, 6)
    for dim, blocks in pieces:
        steps = jnp.exp(jax.random.uniform(jax.random.fold_in(own, dim), (blocks,), jnp.float32, smallest / len(pieces), top_value / len(pieces)))
        gain = gain * jnp.repeat(steps, shape[dim] // blocks).reshape([-1 if axis == dim else 1 for axis in range(len(shape))])
    return gain


def bell_draw(rng, dims, scale, limit, cuts=(), kind=jnp.bfloat16):
    level = levels(rng, dims, cuts, -0.22, 0.18) if cuts else 1.0
    entries = jax.random.normal(rng, dims, jnp.float32) * scale * level
    return jnp.minimum(jnp.maximum(entries, -limit), limit).astype(kind)


def setup_inputs(seed: int = 0) -> dict:
    seeds = jax.random.split(jax.random.key(seed), 6)
    return {
        "blocks": bell_draw(seeds[0], (RGROUPS, CGROUPS, NB_DEV, BQ, BD * BK), 1.0, 6.0, ((0, 16), (1, 16))),
        "coords": draw_coords(jax.random.fold_in(seeds[5], 71), 0),
        "counts": draw_counts(jax.random.fold_in(seeds[5], 71), 0),
        "doc_factor": bell_draw(seeds[3], (DOCS, R), 1.0, 6.0, ((0, 256),)),
        "ctx_factor": bell_draw(seeds[4], (CTX, R), (BD * BK) ** -0.5, 0.0625, ((0, 16),)),
    }


def reference(blocks, coords, counts, doc_factor, ctx_factor):
    total_slots = RGROUPS * CGROUPS * NB_DEV
    flat_blocks = blocks.reshape(total_slots, BQ, BD * BK)
    flat_coords = coords.reshape(total_slots, 3)

    def step(carry, index):
        group = index // NB_DEV
        slot = index % NB_DEV
        prow = group // CGROUPS
        pcol = group % CGROUPS
        place = flat_coords[index]
        valid = slot < counts[prow, pcol]
        qstart = ((prow * QB_ROW + place[0]) * BQ).astype(jnp.int32)
        dstart = ((pcol * DB_COL + place[1]) * BD).astype(jnp.int32)
        kstart = (place[2] * BK).astype(jnp.int32)
        brows = lax.dynamic_slice_in_dim(doc_factor, dstart, BD, 0).astype(jnp.float32)
        crows = lax.dynamic_slice_in_dim(ctx_factor, kstart, BK, 0).astype(jnp.float32)
        table = (brows[:, None, :] * crows[None, :, :]).reshape(BD * BK, R).astype(jnp.bfloat16)
        term = jnp.dot(flat_blocks[index], table, preferred_element_type=jnp.float32)
        term = jnp.where(valid, term, jnp.float32(0.0))
        current = lax.dynamic_slice_in_dim(carry, qstart, BQ, 0)
        carry = lax.dynamic_update_slice_in_dim(carry, current + term, qstart, 0)
        return carry, None

    start = jnp.zeros((QUERIES, R), jnp.float32)
    result, _ = lax.scan(step, start, jnp.arange(total_slots, dtype=jnp.int32))
    return result
```

```python
import jax
import jax.numpy as jnp
from jax import lax
from jax.sharding import PartitionSpec as P

BQ = 128
BD = 128
BK = 64
QBC = 1


def kr_table(brows, crows):
    table = brows[:, None, :].astype(jnp.float32) * crows[None, :, :].astype(jnp.float32)
    return table.reshape(brows.shape[0] * crows.shape[0], brows.shape[1]).astype(jnp.bfloat16)


def gather_rows(piece, axis):
    copies = jnp.broadcast_to(piece[None], (lax.axis_size(axis),) + piece.shape)
    gathered = lax.all_to_all(copies, axis, 0, 0, tiled=True)
    return gathered.reshape(-1, piece.shape[-1])


def body(blocks, coords, counts, doc_factor, ctx_factor):
    doc_slab = gather_rows(doc_factor, "row")
    ctx_all = gather_rows(ctx_factor, "col")
    own_blocks = blocks[0, 0]
    own_coords = coords[0, 0]
    used = counts[0, 0]
    rank = doc_slab.shape[1]
    dev_rows = QBC * BQ
    all_rows = dev_rows * lax.axis_size("col")
    start = jnp.int32(0)
    empty = jnp.zeros((all_rows, rank), jnp.float32)

    def step(index, acc):
        place = own_coords[index]
        qstart = place[0] * BQ
        inside = jnp.logical_and(qstart >= start, qstart < start + all_rows)

        def add_term(inner):
            brows = lax.dynamic_slice_in_dim(doc_slab, place[1] * BD, BD, 0)
            crows = lax.dynamic_slice_in_dim(ctx_all, place[2] * BK, BK, 0)
            term = jnp.dot(
                own_blocks[index], kr_table(brows, crows), preferred_element_type=jnp.float32
            )
            local = jnp.clip(qstart, 0, all_rows - BQ)
            current = lax.dynamic_slice_in_dim(inner, local, BQ, 0)
            return lax.dynamic_update_slice_in_dim(inner, current + term, local, 0)

        return lax.cond(inside, add_term, lambda inner: inner, acc)

    partial_value = lax.fori_loop(0, used, step, empty)
    parts = partial_value.reshape(lax.axis_size("col"), dev_rows, rank)
    return lax.all_to_all(parts, "col", 0, 0, tiled=True).sum(axis=0)


def solution(mesh):
    placed = (
        P("row", "col", None, None, None),
        P("row", "col", None, None),
        P("row", "col"),
        P(("col", "row"), None),
        P("col", None),
    )
    return jax.shard_map(
        body, mesh=mesh, in_specs=placed, out_specs=P(("row", "col"), None), check_vma=False
    )
```

```python
import jax
import jax.numpy as jnp
from jax import lax
from jax.experimental import pallas as pl
from jax.experimental.pallas import tpu as pltpu
from jax.sharding import PartitionSpec as P

BQ = 128
BD = 128
BK = 64
QBC = 1
DOC_CHUNK = 16


def gather_rows(piece, axis):
    copies = jnp.broadcast_to(piece[None], (lax.axis_size(axis),) + piece.shape)
    gathered = lax.all_to_all(copies, axis, 0, 0, tiled=True)
    return gathered.reshape(-1, piece.shape[-1])


def slot_kernel(coords_ref, count_ref, blocks_ref, doc_ref, ctx_ref, out_ref):
    slot = pl.program_id(0)
    n_doc = doc_ref.shape[0]
    n_ctx = ctx_ref.shape[0]
    n_q = out_ref.shape[0]

    @pl.when(slot == 0)
    def _():
        out_ref[...] = jnp.zeros_like(out_ref)

    @pl.when(slot < count_ref[0])
    def _():
        qid = jnp.clip(coords_ref[slot * 3], 0, n_q - 1)
        did = jnp.clip(coords_ref[slot * 3 + 1], 0, n_doc - 1)
        kid = jnp.clip(coords_ref[slot * 3 + 2], 0, n_ctx - 1)
        crows = ctx_ref[kid].astype(jnp.float32)
        width = DOC_CHUNK * BK
        acc = jnp.zeros(out_ref.shape[1:], jnp.float32)
        for chunk in range(BD // DOC_CHUNK):
            brows = doc_ref[did, pl.ds(chunk * DOC_CHUNK, DOC_CHUNK), :].astype(jnp.float32)
            table = (brows[:, None, :] * crows[None, :, :]).reshape(width, crows.shape[-1])
            acc += jnp.dot(
                blocks_ref[:, pl.ds(chunk * width, width)],
                table.astype(jnp.bfloat16),
                preferred_element_type=jnp.float32,
            )
        out_ref[qid] += acc


def slot_terms(own_blocks, own_coords, used, doc_blocks, ctx_blocks, n_q):
    slots, rows, width = own_blocks.shape
    rank = doc_blocks.shape[-1]

    def block_map(s, coords_ref, count_ref):
        return (jnp.minimum(s, jnp.maximum(count_ref[0] - 1, 0)), 0, 0)

    grid_spec = pltpu.PrefetchScalarGridSpec(
        num_scalar_prefetch=2,
        grid=(slots,),
        in_specs=[
            pl.BlockSpec((None, rows, width), block_map),
            pl.BlockSpec(doc_blocks.shape, lambda s, c, n: (0, 0, 0)),
            pl.BlockSpec(ctx_blocks.shape, lambda s, c, n: (0, 0, 0)),
        ],
        out_specs=pl.BlockSpec((n_q, rows, rank), lambda s, c, n: (0, 0, 0)),
    )
    cost = pl.CostEstimate(
        flops=2 * slots * rows * width * rank,
        bytes_accessed=own_blocks.size * 2 + n_q * rows * rank * 4,
        transcendentals=0,
    )
    return pl.pallas_call(
        slot_kernel,
        grid_spec=grid_spec,
        out_shape=jax.ShapeDtypeStruct((n_q, rows, rank), jnp.float32),
        compiler_params=pltpu.CompilerParams(dimension_semantics=("arbitrary",)),
        cost_estimate=cost,
    )(own_coords.reshape(-1), used.reshape(-1), own_blocks, doc_blocks, ctx_blocks)


def body(blocks, coords, counts, doc_factor, ctx_factor):
    doc_slab = gather_rows(doc_factor, "row")
    ctx_all = gather_rows(ctx_factor, "col")
    rank = doc_slab.shape[1]
    n_q = QBC * lax.axis_size("col")
    doc_blocks = doc_slab.reshape(-1, BD, rank)
    ctx_blocks = ctx_all.reshape(-1, BK, rank)
    parts = slot_terms(blocks[0, 0], coords[0, 0], counts[0], doc_blocks, ctx_blocks, n_q)
    return lax.all_to_all(parts, "col", 0, 0, tiled=True).sum(axis=0)


def solution(mesh):
    placed = (
        P("row", "col", None, None, None),
        P("row", "col", None, None),
        P("row", "col"),
        P(("col", "row"), None),
        P("col", None),
    )
    return jax.shard_map(
        body, mesh=mesh, in_specs=placed, out_specs=P(("row", "col"), None), check_vma=False
    )
```

```python
import jax
import jax.numpy as jnp
from jax import lax
from jax.experimental import pallas as pl
from jax.experimental.pallas import tpu as pltpu
from jax.sharding import PartitionSpec as P

BQ = 128
BD = 128
BK = 64
QBC = 1
DOC_CHUNK = 16


def gather_rows(piece, axis):
    copies = jnp.broadcast_to(piece[None], (lax.axis_size(axis),) + piece.shape)
    gathered = lax.all_to_all(copies, axis, 0, 0, tiled=True)
    return gathered.reshape(-1, piece.shape[-1])


def slot_kernel(coords_ref, count_ref, blocks_ref, doc_ref, ctx_ref, out_ref):
    slot = pl.program_id(0)
    n_doc = doc_ref.shape[0]
    n_ctx = ctx_ref.shape[0]
    n_q = out_ref.shape[0]

    @pl.when(slot == 0)
    def _():
        out_ref[...] = jnp.zeros_like(out_ref)

    @pl.when(slot < count_ref[0])
    def _():
        qid = jnp.clip(coords_ref[slot * 3], 0, n_q - 1)
        did = jnp.clip(coords_ref[slot * 3 + 1], 0, n_doc - 1)
        kid = jnp.clip(coords_ref[slot * 3 + 2], 0, n_ctx - 1)
        crows = ctx_ref[kid]
        width = DOC_CHUNK * BK
        acc = jnp.zeros(out_ref.shape[1:], jnp.float32)
        for chunk in range(BD // DOC_CHUNK):
            brows = doc_ref[did, pl.ds(chunk * DOC_CHUNK, DOC_CHUNK), :]
            table = (brows[:, None, :] * crows[None, :, :]).reshape(width, crows.shape[-1])
            acc += jnp.dot(
                blocks_ref[:, pl.ds(chunk * width, width)],
                table,
                preferred_element_type=jnp.float32,
            )
        out_ref[qid] += acc


def slot_terms(own_blocks, own_coords, used, doc_blocks, ctx_blocks, n_q):
    slots, rows, width = own_blocks.shape
    rank = doc_blocks.shape[-1]

    def block_map(s, coords_ref, count_ref):
        return (jnp.minimum(s, jnp.maximum(count_ref[0] - 1, 0)), 0, 0)

    grid_spec = pltpu.PrefetchScalarGridSpec(
        num_scalar_prefetch=2,
        grid=(slots,),
        in_specs=[
            pl.BlockSpec((None, rows, width), block_map),
            pl.BlockSpec(doc_blocks.shape, lambda s, c, n: (0, 0, 0)),
            pl.BlockSpec(ctx_blocks.shape, lambda s, c, n: (0, 0, 0)),
        ],
        out_specs=pl.BlockSpec((n_q, rows, rank), lambda s, c, n: (0, 0, 0)),
    )
    cost = pl.CostEstimate(
        flops=2 * slots * rows * width * rank,
        bytes_accessed=own_blocks.size * 2 + n_q * rows * rank * 4,
        transcendentals=0,
    )
    return pl.pallas_call(
        slot_kernel,
        grid_spec=grid_spec,
        out_shape=jax.ShapeDtypeStruct((n_q, rows, rank), jnp.float32),
        compiler_params=pltpu.CompilerParams(dimension_semantics=("arbitrary",)),
        cost_estimate=cost,
    )(own_coords.reshape(-1), used.reshape(-1), own_blocks, doc_blocks, ctx_blocks)


def body(blocks, coords, counts, doc_factor, ctx_factor):
    doc_slab = lax.all_gather(doc_factor, "row", axis=0, tiled=True)
    ctx_all = gather_rows(ctx_factor, "col")
    rank = doc_slab.shape[1]
    n_q = QBC * lax.axis_size("col")
    doc_blocks = doc_slab.reshape(-1, BD, rank)
    ctx_blocks = ctx_all.reshape(-1, BK, rank)
    parts = slot_terms(blocks[0, 0], coords[0, 0], counts[0], doc_blocks, ctx_blocks, n_q)
    return lax.all_to_all(parts, "col", 0, 0, tiled=True).sum(axis=0)


def solution(mesh):
    placed = (
        P("row", "col", None, None, None),
        P("row", "col", None, None),
        P("row", "col"),
        P(("col", "row"), None),
        P("col", None),
    )
    return jax.shard_map(
        body, mesh=mesh, in_specs=placed, out_specs=P(("row", "col"), None), check_vma=False
    )
```

```python
import jax
import jax.numpy as jnp
from jax import lax
from jax.experimental import pallas as pl
from jax.experimental.pallas import tpu as pltpu
from jax.sharding import PartitionSpec as P

BQ = 128
BD = 128
BK = 64
QBC = 1
DOC_CHUNK = 16


def gather_rows(piece, axis):
    copies = jnp.broadcast_to(piece[None], (lax.axis_size(axis),) + piece.shape)
    gathered = lax.all_to_all(copies, axis, 0, 0, tiled=True)
    return gathered.reshape(-1, piece.shape[-1])


def slot_kernel(coords_ref, count_ref, blocks_hbm, doc_ref, ctx_ref, out_ref, held, sems):
    n_doc = doc_ref.shape[0]
    n_ctx = ctx_ref.shape[0]
    n_q = out_ref.shape[0]
    slots = blocks_hbm.shape[0]
    pieces = held.shape[1]
    piece = held.shape[-1]
    used = jnp.clip(count_ref[0], 0, slots)

    def fetch(slot, part):
        return pltpu.make_async_copy(
            blocks_hbm.at[slot, :, pl.ds(part * piece, piece)],
            held.at[slot % 2, part],
            sems.at[slot % 2, part],
        )

    @pl.when(used > 0)
    def _():
        for part in range(pieces):
            fetch(0, part).start()

    out_ref[...] = jnp.zeros_like(out_ref)

    def step(slot, carry):
        @pl.when(slot + 1 < used)
        def _():
            for part in range(pieces):
                fetch(slot + 1, part).start()

        qid = jnp.clip(coords_ref[0, slot], 0, n_q - 1)
        did = jnp.clip(coords_ref[1, slot], 0, n_doc - 1)
        kid = jnp.clip(coords_ref[2, slot], 0, n_ctx - 1)
        crows = ctx_ref[kid]
        width = DOC_CHUNK * BK
        acc = jnp.zeros(out_ref.shape[1:], jnp.float32)
        for part in range(pieces):
            fetch(slot, part).wait()
            for sub in range(piece // width):
                first = (part * piece + sub * width) // BK
                brows = doc_ref[did, pl.ds(first, DOC_CHUNK), :]
                table = (brows[:, None, :] * crows[None, :, :]).reshape(width, crows.shape[-1])
                acc += jnp.dot(
                    held[slot % 2, part, :, pl.ds(sub * width, width)],
                    table,
                    preferred_element_type=jnp.float32,
                )
        out_ref[qid] += acc
        return carry

    lax.fori_loop(0, used, step, 0)


def slot_terms(own_blocks, own_coords, used, doc_blocks, ctx_blocks, n_q):
    slots, rows, width = own_blocks.shape
    rank = doc_blocks.shape[-1]
    pieces = 4
    cost = pl.CostEstimate(
        flops=2 * slots * rows * width * rank,
        bytes_accessed=own_blocks.size * 2 + n_q * rows * rank * 4,
        transcendentals=0,
    )
    return pl.pallas_call(
        slot_kernel,
        in_specs=[
            pl.BlockSpec(memory_space=pltpu.SMEM),
            pl.BlockSpec(memory_space=pltpu.SMEM),
            pl.BlockSpec(memory_space=pl.ANY),
            pl.BlockSpec(memory_space=pltpu.VMEM),
            pl.BlockSpec(memory_space=pltpu.VMEM),
        ],
        out_specs=pl.BlockSpec(memory_space=pltpu.VMEM),
        out_shape=jax.ShapeDtypeStruct((n_q, rows, rank), jnp.float32),
        scratch_shapes=[
            pltpu.VMEM((2, pieces, rows, width // pieces), own_blocks.dtype),
            pltpu.SemaphoreType.DMA((2, pieces)),
        ],
        cost_estimate=cost,
    )(own_coords.T, used.reshape(-1), own_blocks, doc_blocks, ctx_blocks)


def body(blocks, coords, counts, doc_factor, ctx_factor):
    doc_slab = lax.all_gather(doc_factor, "row", axis=0, tiled=True)
    ctx_all = gather_rows(ctx_factor, "col")
    rank = doc_slab.shape[1]
    n_q = QBC * lax.axis_size("col")
    doc_blocks = doc_slab.reshape(-1, BD, rank)
    ctx_blocks = ctx_all.reshape(-1, BK, rank)
    parts = slot_terms(blocks[0, 0], coords[0, 0], counts[0], doc_blocks, ctx_blocks, n_q)
    return lax.all_to_all(parts, "col", 0, 0, tiled=True).sum(axis=0)


def solution(mesh):
    placed = (
        P("row", "col", None, None, None),
        P("row", "col", None, None),
        P("row", "col"),
        P(("col", "row"), None),
        P("col", None),
    )
    return jax.shard_map(
        body, mesh=mesh, in_specs=placed, out_specs=P(("row", "col"), None), check_vma=False
    )
```

```python
import jax
import jax.numpy as jnp
from jax import lax
from jax.experimental import pallas as pl
from jax.experimental.pallas import tpu as pltpu
from jax.sharding import PartitionSpec as P

BQ = 128
BD = 128
BK = 64
QBC = 1
DOC_CHUNK = 16


def gather_rows(piece, axis):
    copies = jnp.broadcast_to(piece[None], (lax.axis_size(axis),) + piece.shape)
    gathered = lax.all_to_all(copies, axis, 0, 0, tiled=True)
    return gathered.reshape(-1, piece.shape[-1])


def slot_kernel(coords_ref, blocks_hbm, doc_ref, ctx_ref, out_ref, held, sems):
    n_doc = doc_ref.shape[0]
    n_ctx = ctx_ref.shape[0]
    n_q = out_ref.shape[0]
    slots = blocks_hbm.shape[0]
    pieces = held.shape[1]
    piece = held.shape[-1]
    used = jnp.clip(coords_ref[3, 0], 0, slots)

    def fetch(slot, part):
        return pltpu.make_async_copy(
            blocks_hbm.at[slot, :, pl.ds(part * piece, piece)],
            held.at[slot % 2, part],
            sems.at[slot % 2, part],
        )

    @pl.when(used > 0)
    def _():
        for part in range(pieces):
            fetch(0, part).start()

    out_ref[...] = jnp.zeros_like(out_ref)

    def step(slot, carry):
        @pl.when(slot + 1 < used)
        def _():
            for part in range(pieces):
                fetch(slot + 1, part).start()

        qid = jnp.clip(coords_ref[0, slot], 0, n_q - 1)
        did = jnp.clip(coords_ref[1, slot], 0, n_doc - 1)
        kid = jnp.clip(coords_ref[2, slot], 0, n_ctx - 1)
        crows = ctx_ref[kid]
        width = DOC_CHUNK * BK
        acc = jnp.zeros(out_ref.shape[1:], jnp.float32)
        for part in range(pieces):
            fetch(slot, part).wait()
            for sub in range(piece // width):
                first = (part * piece + sub * width) // BK
                brows = doc_ref[did, pl.ds(first, DOC_CHUNK), :]
                table = (brows[:, None, :] * crows[None, :, :]).reshape(width, crows.shape[-1])
                acc += jnp.dot(
                    held[slot % 2, part, :, pl.ds(sub * width, width)],
                    table,
                    preferred_element_type=jnp.float32,
                )
        out_ref[qid] += acc
        return carry

    lax.fori_loop(0, used, step, 0)


def slot_terms(own_blocks, table, doc_blocks, ctx_blocks, n_q):
    slots, rows, width = own_blocks.shape
    rank = doc_blocks.shape[-1]
    pieces = 4
    cost = pl.CostEstimate(
        flops=2 * slots * rows * width * rank,
        bytes_accessed=own_blocks.size * 2 + n_q * rows * rank * 4,
        transcendentals=0,
    )
    return pl.pallas_call(
        slot_kernel,
        in_specs=[
            pl.BlockSpec(memory_space=pltpu.SMEM),
            pl.BlockSpec(memory_space=pl.ANY),
            pl.BlockSpec(memory_space=pltpu.VMEM),
            pl.BlockSpec(memory_space=pltpu.VMEM),
        ],
        out_specs=pl.BlockSpec(memory_space=pltpu.VMEM),
        out_shape=jax.ShapeDtypeStruct((n_q, rows, rank), jnp.float32),
        scratch_shapes=[
            pltpu.VMEM((2, pieces, rows, width // pieces), own_blocks.dtype),
            pltpu.SemaphoreType.DMA((2, pieces)),
        ],
        cost_estimate=cost,
    )(table, own_blocks, doc_blocks, ctx_blocks)


def slot_table(coords, counts):
    ids = coords[0, 0].T
    used = jnp.broadcast_to(counts[0].reshape(1, 1), (1, ids.shape[1]))
    return jnp.concatenate([ids, used], axis=0)


def body(blocks, coords, counts, doc_factor, ctx_factor):
    table = slot_table(coords, counts)
    table, ctx_factor = lax.optimization_barrier((table, ctx_factor))
    doc_slab = lax.all_gather(doc_factor, "row", axis=0, tiled=True)
    ctx_all = gather_rows(ctx_factor, "col")
    rank = doc_slab.shape[1]
    n_q = QBC * lax.axis_size("col")
    doc_blocks = doc_slab.reshape(-1, BD, rank)
    ctx_blocks = ctx_all.reshape(-1, BK, rank)
    parts = slot_terms(blocks[0, 0], table, doc_blocks, ctx_blocks, n_q)
    return lax.all_to_all(parts, "col", 0, 0, tiled=True).sum(axis=0)


def solution(mesh):
    placed = (
        P("row", "col", None, None, None),
        P("row", "col", None, None),
        P("row", "col"),
        P(("col", "row"), None),
        P("col", None),
    )
    return jax.shard_map(
        body, mesh=mesh, in_specs=placed, out_specs=P(("row", "col"), None), check_vma=False
    )
```

```python
import jax
import jax.numpy as jnp
from jax import lax
from jax.experimental import pallas as pl
from jax.experimental.pallas import tpu as pltpu
from jax.sharding import PartitionSpec as P

BQ = 128
BD = 128
BK = 64
QBC = 1
DOC_CHUNK = 16
VMEM_LIMIT = 50 * 1024 * 1024


def gather_rows(piece, axis):
    copies = jnp.broadcast_to(piece[None], (lax.axis_size(axis),) + piece.shape)
    gathered = lax.all_to_all(copies, axis, 0, 0, tiled=True)
    return gathered.reshape(-1, piece.shape[-1])


def slot_kernel(coords_ref, count_ref, blocks_hbm, doc_ref, ctx_ref, out_ref, held, sems):
    n_doc = doc_ref.shape[0]
    n_ctx = ctx_ref.shape[0]
    n_q = out_ref.shape[0]
    slots = blocks_hbm.shape[0]
    pieces = held.shape[1]
    piece = held.shape[-1]
    used = jnp.clip(count_ref[0], 0, slots)

    def fetch(slot, part):
        return pltpu.make_async_copy(
            blocks_hbm.at[slot, :, pl.ds(part * piece, piece)],
            held.at[slot % 2, part],
            sems.at[slot % 2, part],
        )

    @pl.when(used > 0)
    def _():
        for part in range(pieces):
            fetch(0, part).start()

    out_ref[...] = jnp.zeros_like(out_ref)

    def step(slot, carry):
        @pl.when(slot + 1 < used)
        def _():
            for part in range(pieces):
                fetch(slot + 1, part).start()

        qid = jnp.clip(coords_ref[0, slot], 0, n_q - 1)
        did = jnp.clip(coords_ref[1, slot], 0, n_doc - 1)
        kid = jnp.clip(coords_ref[2, slot], 0, n_ctx - 1)
        crows = ctx_ref[kid]
        width = DOC_CHUNK * BK
        acc = jnp.zeros(out_ref.shape[1:], jnp.float32)
        for part in range(pieces):
            fetch(slot, part).wait()
            for sub in range(piece // width):
                first = (part * piece + sub * width) // BK
                brows = doc_ref[did, pl.ds(first, DOC_CHUNK), :]
                table = (brows[:, None, :] * crows[None, :, :]).reshape(width, crows.shape[-1])
                acc += jnp.dot(
                    held[slot % 2, part, :, pl.ds(sub * width, width)],
                    table,
                    preferred_element_type=jnp.float32,
                )
        out_ref[qid] += acc
        return carry

    lax.fori_loop(0, used, step, 0)


def slot_terms(own_blocks, own_coords, used, doc_blocks, ctx_blocks, n_q):
    slots, rows, width = own_blocks.shape
    rank = doc_blocks.shape[-1]
    pieces = 4
    cost = pl.CostEstimate(
        flops=2 * slots * rows * width * rank,
        bytes_accessed=own_blocks.size * 2 + n_q * rows * rank * 4,
        transcendentals=0,
    )
    return pl.pallas_call(
        slot_kernel,
        in_specs=[
            pl.BlockSpec(memory_space=pltpu.SMEM),
            pl.BlockSpec(memory_space=pltpu.SMEM),
            pl.BlockSpec(memory_space=pl.ANY),
            pl.BlockSpec(memory_space=pltpu.VMEM),
            pl.BlockSpec(memory_space=pltpu.VMEM),
        ],
        out_specs=pl.BlockSpec(memory_space=pltpu.VMEM),
        out_shape=jax.ShapeDtypeStruct((n_q, rows, rank), jnp.float32),
        scratch_shapes=[
            pltpu.VMEM((2, pieces, rows, width // pieces), own_blocks.dtype),
            pltpu.SemaphoreType.DMA((2, pieces)),
        ],
        compiler_params=pltpu.CompilerParams(vmem_limit_bytes=VMEM_LIMIT),
        cost_estimate=cost,
    )(own_coords.T, used.reshape(-1), own_blocks, doc_blocks, ctx_blocks)


def body(blocks, coords, counts, doc_factor, ctx_factor):
    doc_slab = lax.all_gather(doc_factor, "row", axis=0, tiled=True)
    ctx_all = gather_rows(ctx_factor, "col")
    rank = doc_slab.shape[1]
    n_q = QBC * lax.axis_size("col")
    doc_blocks = doc_slab.reshape(-1, BD, rank)
    ctx_blocks = ctx_all.reshape(-1, BK, rank)
    parts = slot_terms(blocks[0, 0], coords[0, 0], counts[0], doc_blocks, ctx_blocks, n_q)
    return lax.all_to_all(parts, "col", 0, 0, tiled=True).sum(axis=0)


def solution(mesh):
    placed = (
        P("row", "col", None, None, None),
        P("row", "col", None, None),
        P("row", "col"),
        P(("col", "row"), None),
        P("col", None),
    )
    return jax.shard_map(
        body, mesh=mesh, in_specs=placed, out_specs=P(("row", "col"), None), check_vma=False
    )
```

```python
import jax
import jax.numpy as jnp
from jax import lax
from jax.experimental import pallas as pl
from jax.experimental.pallas import tpu as pltpu
from jax.sharding import PartitionSpec as P

BQ = 128
BD = 128
BK = 64
QBC = 1
DOC_CHUNK = 16
VMEM_LIMIT = 50 * 1024 * 1024


def gather_rows(piece, axis):
    copies = jnp.broadcast_to(piece[None], (lax.axis_size(axis),) + piece.shape)
    gathered = lax.all_to_all(copies, axis, 0, 0, tiled=True)
    return gathered.reshape(-1, piece.shape[-1])


def slot_kernel(coords_ref, count_ref, blocks_hbm, doc_ref, ctx_ref, out_ref, held, sems):
    n_doc = doc_ref.shape[0]
    n_ctx = ctx_ref.shape[0]
    n_q = out_ref.shape[0]
    slots = blocks_hbm.shape[0]
    pieces = held.shape[1]
    piece = held.shape[-1]
    used = jnp.clip(count_ref[0], 0, slots)

    def fetch(slot, part):
        return pltpu.make_async_copy(
            blocks_hbm.at[slot, :, pl.ds(part * piece, piece)],
            held.at[slot % 2, part],
            sems.at[slot % 2, part],
        )

    @pl.when(used > 0)
    def _():
        for part in range(pieces):
            fetch(0, part).start()

    out_ref[...] = jnp.zeros_like(out_ref)

    def step(slot, carry):
        @pl.when(slot + 1 < used)
        def _():
            for part in range(pieces):
                fetch(slot + 1, part).start()

        qid = jnp.clip(coords_ref[0, slot], 0, n_q - 1)
        did = jnp.clip(coords_ref[1, slot], 0, n_doc - 1)
        kid = jnp.clip(coords_ref[2, slot], 0, n_ctx - 1)
        crows = ctx_ref[kid]
        width = DOC_CHUNK * BK
        acc = jnp.zeros(out_ref.shape[1:], jnp.float32)
        for part in range(pieces):
            fetch(slot, part).wait()
            for sub in range(piece // width):
                first = (part * piece + sub * width) // BK
                brows = doc_ref[did, pl.ds(first, DOC_CHUNK), :]
                table = (brows[:, None, :] * crows[None, :, :]).reshape(width, crows.shape[-1])
                acc += jnp.dot(
                    held[slot % 2, part, :, pl.ds(sub * width, width)],
                    table,
                    preferred_element_type=jnp.float32,
                )
        out_ref[qid] += acc
        return carry

    lax.fori_loop(0, used, step, 0)


def slot_terms(own_blocks, own_coords, used, doc_blocks, ctx_blocks, n_q):
    slots, rows, width = own_blocks.shape
    rank = doc_blocks.shape[-1]
    pieces = 2
    cost = pl.CostEstimate(
        flops=2 * slots * rows * width * rank,
        bytes_accessed=own_blocks.size * 2 + n_q * rows * rank * 4,
        transcendentals=0,
    )
    return pl.pallas_call(
        slot_kernel,
        in_specs=[
            pl.BlockSpec(memory_space=pltpu.SMEM),
            pl.BlockSpec(memory_space=pltpu.SMEM),
            pl.BlockSpec(memory_space=pl.ANY),
            pl.BlockSpec(memory_space=pltpu.VMEM),
            pl.BlockSpec(memory_space=pltpu.VMEM),
        ],
        out_specs=pl.BlockSpec(memory_space=pltpu.VMEM),
        out_shape=jax.ShapeDtypeStruct((n_q, rows, rank), jnp.float32),
        scratch_shapes=[
            pltpu.VMEM((2, pieces, rows, width // pieces), own_blocks.dtype),
            pltpu.SemaphoreType.DMA((2, pieces)),
        ],
        compiler_params=pltpu.CompilerParams(vmem_limit_bytes=VMEM_LIMIT),
        cost_estimate=cost,
    )(own_coords.T, used.reshape(-1), own_blocks, doc_blocks, ctx_blocks)


def body(blocks, coords, counts, doc_factor, ctx_factor):
    doc_slab = lax.all_gather(doc_factor, "row", axis=0, tiled=True)
    ctx_all = gather_rows(ctx_factor, "col")
    rank = doc_slab.shape[1]
    n_q = QBC * lax.axis_size("col")
    doc_blocks = doc_slab.reshape(-1, BD, rank)
    ctx_blocks = ctx_all.reshape(-1, BK, rank)
    parts = slot_terms(blocks[0, 0], coords[0, 0], counts[0], doc_blocks, ctx_blocks, n_q)
    return lax.all_to_all(parts, "col", 0, 0, tiled=True).sum(axis=0)


def solution(mesh):
    placed = (
        P("row", "col", None, None, None),
        P("row", "col", None, None),
        P("row", "col"),
        P(("col", "row"), None),
        P("col", None),
    )
    return jax.shard_map(
        body, mesh=mesh, in_specs=placed, out_specs=P(("row", "col"), None), check_vma=False
    )
```

```python
import jax
import jax.numpy as jnp
from jax import lax
from jax.experimental import pallas as pl
from jax.experimental.pallas import tpu as pltpu
from jax.sharding import PartitionSpec as P

BQ = 128
BD = 128
BK = 64
QBC = 1
DOC_CHUNK = 16
VMEM_LIMIT = 50 * 1024 * 1024


def gather_rows(piece, axis):
    copies = jnp.broadcast_to(piece[None], (lax.axis_size(axis),) + piece.shape)
    gathered = lax.all_to_all(copies, axis, 0, 0, tiled=True)
    return gathered.reshape(-1, piece.shape[-1])


def slot_kernel(coords_ref, count_ref, blocks_hbm, doc_ref, ctx_ref, out_ref, held, sems):
    n_doc = doc_ref.shape[0]
    n_ctx = ctx_ref.shape[0]
    n_q = out_ref.shape[0]
    slots = blocks_hbm.shape[0]
    pieces = held.shape[1]
    piece = held.shape[-1]
    used = jnp.clip(count_ref[0], 0, slots)

    def fetch(slot, part):
        return pltpu.make_async_copy(
            blocks_hbm.at[slot, :, pl.ds(part * piece, piece)],
            held.at[slot % 2, part],
            sems.at[slot % 2, part],
        )

    @pl.when(used > 0)
    def _():
        for part in range(pieces):
            fetch(0, part).start()

    out_ref[...] = jnp.zeros_like(out_ref)

    def step(slot, carry):
        @pl.when(slot + 1 < used)
        def _():
            for part in range(pieces):
                fetch(slot + 1, part).start()

        qid = jnp.clip(coords_ref[0, slot], 0, n_q - 1)
        did = jnp.clip(coords_ref[1, slot], 0, n_doc - 1)
        kid = jnp.clip(coords_ref[2, slot], 0, n_ctx - 1)
        crows = ctx_ref[kid]
        width = DOC_CHUNK * BK
        acc = jnp.zeros(out_ref.shape[1:], jnp.float32)
        for part in range(pieces):
            fetch(slot, part).wait()
            for sub in range(piece // width):
                first = (part * piece + sub * width) // BK
                brows = doc_ref[did, pl.ds(first, DOC_CHUNK), :]
                table = (brows[:, None, :] * crows[None, :, :]).reshape(width, crows.shape[-1])
                acc += jnp.dot(
                    held[slot % 2, part, :, pl.ds(sub * width, width)],
                    table,
                    preferred_element_type=jnp.float32,
                )
        out_ref[qid] += acc
        return carry

    lax.fori_loop(0, used, step, 0)


def slot_terms(own_blocks, own_coords, used, doc_blocks, ctx_blocks, n_q):
    slots, rows, width = own_blocks.shape
    rank = doc_blocks.shape[-1]
    pieces = 1
    cost = pl.CostEstimate(
        flops=2 * slots * rows * width * rank,
        bytes_accessed=own_blocks.size * 2 + n_q * rows * rank * 4,
        transcendentals=0,
    )
    return pl.pallas_call(
        slot_kernel,
        in_specs=[
            pl.BlockSpec(memory_space=pltpu.SMEM),
            pl.BlockSpec(memory_space=pltpu.SMEM),
            pl.BlockSpec(memory_space=pl.ANY),
            pl.BlockSpec(memory_space=pltpu.VMEM),
            pl.BlockSpec(memory_space=pltpu.VMEM),
        ],
        out_specs=pl.BlockSpec(memory_space=pltpu.VMEM),
        out_shape=jax.ShapeDtypeStruct((n_q, rows, rank), jnp.float32),
        scratch_shapes=[
            pltpu.VMEM((2, pieces, rows, width // pieces), own_blocks.dtype),
            pltpu.SemaphoreType.DMA((2, pieces)),
        ],
        compiler_params=pltpu.CompilerParams(vmem_limit_bytes=VMEM_LIMIT),
        cost_estimate=cost,
    )(own_coords.T, used.reshape(-1), own_blocks, doc_blocks, ctx_blocks)


def body(blocks, coords, counts, doc_factor, ctx_factor):
    doc_slab = lax.all_gather(doc_factor, "row", axis=0, tiled=True)
    ctx_all = gather_rows(ctx_factor, "col")
    rank = doc_slab.shape[1]
    n_q = QBC * lax.axis_size("col")
    doc_blocks = doc_slab.reshape(-1, BD, rank)
    ctx_blocks = ctx_all.reshape(-1, BK, rank)
    parts = slot_terms(blocks[0, 0], coords[0, 0], counts[0], doc_blocks, ctx_blocks, n_q)
    return lax.all_to_all(parts, "col", 0, 0, tiled=True).sum(axis=0)


def solution(mesh):
    placed = (
        P("row", "col", None, None, None),
        P("row", "col", None, None),
        P("row", "col"),
        P(("col", "row"), None),
        P("col", None),
    )
    return jax.shard_map(
        body, mesh=mesh, in_specs=placed, out_specs=P(("row", "col"), None), check_vma=False
    )
```

```python
import jax
import jax.numpy as jnp
from jax import lax
from jax.experimental import pallas as pl
from jax.experimental.pallas import tpu as pltpu
from jax.sharding import PartitionSpec as P

BQ = 128
BD = 128
BK = 64
QBC = 1
DOC_CHUNK = 64
VMEM_LIMIT = 50 * 1024 * 1024


def gather_rows(piece, axis):
    copies = jnp.broadcast_to(piece[None], (lax.axis_size(axis),) + piece.shape)
    gathered = lax.all_to_all(copies, axis, 0, 0, tiled=True)
    return gathered.reshape(-1, piece.shape[-1])


def slot_kernel(coords_ref, count_ref, blocks_hbm, doc_ref, ctx_ref, out_ref, held, sems):
    n_doc = doc_ref.shape[0]
    n_ctx = ctx_ref.shape[0]
    n_q = out_ref.shape[0]
    slots = blocks_hbm.shape[0]
    pieces = held.shape[1]
    piece = held.shape[-1]
    used = jnp.clip(count_ref[0], 0, slots)

    def fetch(slot, part):
        return pltpu.make_async_copy(
            blocks_hbm.at[slot, :, pl.ds(part * piece, piece)],
            held.at[slot % 2, part],
            sems.at[slot % 2, part],
        )

    @pl.when(used > 0)
    def _():
        for part in range(pieces):
            fetch(0, part).start()

    out_ref[...] = jnp.zeros_like(out_ref)

    def step(slot, carry):
        @pl.when(slot + 1 < used)
        def _():
            for part in range(pieces):
                fetch(slot + 1, part).start()

        qid = jnp.clip(coords_ref[0, slot], 0, n_q - 1)
        did = jnp.clip(coords_ref[1, slot], 0, n_doc - 1)
        kid = jnp.clip(coords_ref[2, slot], 0, n_ctx - 1)
        crows = ctx_ref[kid]
        width = DOC_CHUNK * BK
        acc = jnp.zeros(out_ref.shape[1:], jnp.float32)
        for part in range(pieces):
            fetch(slot, part).wait()
            for sub in range(piece // width):
                first = (part * piece + sub * width) // BK
                brows = doc_ref[did, pl.ds(first, DOC_CHUNK), :]
                table = (brows[:, None, :] * crows[None, :, :]).reshape(width, crows.shape[-1])
                acc += jnp.dot(
                    held[slot % 2, part, :, pl.ds(sub * width, width)],
                    table,
                    preferred_element_type=jnp.float32,
                )
        out_ref[qid] += acc
        return carry

    lax.fori_loop(0, used, step, 0)


def slot_terms(own_blocks, own_coords, used, doc_blocks, ctx_blocks, n_q):
    slots, rows, width = own_blocks.shape
    rank = doc_blocks.shape[-1]
    pieces = 2
    cost = pl.CostEstimate(
        flops=2 * slots * rows * width * rank,
        bytes_accessed=own_blocks.size * 2 + n_q * rows * rank * 4,
        transcendentals=0,
    )
    return pl.pallas_call(
        slot_kernel,
        in_specs=[
            pl.BlockSpec(memory_space=pltpu.SMEM),
            pl.BlockSpec(memory_space=pltpu.SMEM),
            pl.BlockSpec(memory_space=pl.ANY),
            pl.BlockSpec(memory_space=pltpu.VMEM),
            pl.BlockSpec(memory_space=pltpu.VMEM),
        ],
        out_specs=pl.BlockSpec(memory_space=pltpu.VMEM),
        out_shape=jax.ShapeDtypeStruct((n_q, rows, rank), jnp.float32),
        scratch_shapes=[
            pltpu.VMEM((2, pieces, rows, width // pieces), own_blocks.dtype),
            pltpu.SemaphoreType.DMA((2, pieces)),
        ],
        compiler_params=pltpu.CompilerParams(vmem_limit_bytes=VMEM_LIMIT),
        cost_estimate=cost,
    )(own_coords.T, used.reshape(-1), own_blocks, doc_blocks, ctx_blocks)


def body(blocks, coords, counts, doc_factor, ctx_factor):
    doc_slab = lax.all_gather(doc_factor, "row", axis=0, tiled=True)
    ctx_all = gather_rows(ctx_factor, "col")
    rank = doc_slab.shape[1]
    n_q = QBC * lax.axis_size("col")
    doc_blocks = doc_slab.reshape(-1, BD, rank)
    ctx_blocks = ctx_all.reshape(-1, BK, rank)
    parts = slot_terms(blocks[0, 0], coords[0, 0], counts[0], doc_blocks, ctx_blocks, n_q)
    return lax.all_to_all(parts, "col", 0, 0, tiled=True).sum(axis=0)


def solution(mesh):
    placed = (
        P("row", "col", None, None, None),
        P("row", "col", None, None),
        P("row", "col"),
        P(("col", "row"), None),
        P("col", None),
    )
    return jax.shard_map(
        body, mesh=mesh, in_specs=placed, out_specs=P(("row", "col"), None), check_vma=False
    )
```

```python
import jax
import jax.numpy as jnp
from jax import lax
from jax.experimental import pallas as pl
from jax.experimental.pallas import tpu as pltpu
from jax.sharding import PartitionSpec as P

BQ = 128
BD = 128
BK = 64
QBC = 1
DOC_CHUNK = 16
VMEM_LIMIT = 50 * 1024 * 1024


def gather_rows(piece, axis):
    copies = jnp.broadcast_to(piece[None], (lax.axis_size(axis),) + piece.shape)
    gathered = lax.all_to_all(copies, axis, 0, 0, tiled=True)
    return gathered.reshape(-1, piece.shape[-1])


def slot_kernel(coords_ref, blocks_hbm, doc_ref, ctx_ref, out_ref, held, sems):
    n_doc = doc_ref.shape[0]
    n_ctx = ctx_ref.shape[0]
    n_q = out_ref.shape[0]
    slots = blocks_hbm.shape[0]
    pieces = held.shape[1]
    piece = held.shape[-1]
    used = jnp.clip(coords_ref[3, 0], 0, slots)

    def fetch(slot, part):
        return pltpu.make_async_copy(
            blocks_hbm.at[slot, :, pl.ds(part * piece, piece)],
            held.at[slot % 2, part],
            sems.at[slot % 2, part],
        )

    @pl.when(used > 0)
    def _():
        for part in range(pieces):
            fetch(0, part).start()

    out_ref[...] = jnp.zeros_like(out_ref)

    def step(slot, carry):
        @pl.when(slot + 1 < used)
        def _():
            for part in range(pieces):
                fetch(slot + 1, part).start()

        qid = jnp.clip(coords_ref[0, slot], 0, n_q - 1)
        did = jnp.clip(coords_ref[1, slot], 0, n_doc - 1)
        kid = jnp.clip(coords_ref[2, slot], 0, n_ctx - 1)
        crows = ctx_ref[kid]
        width = DOC_CHUNK * BK
        acc = jnp.zeros(out_ref.shape[1:], jnp.float32)
        for part in range(pieces):
            fetch(slot, part).wait()
            for sub in range(piece // width):
                first = (part * piece + sub * width) // BK
                brows = doc_ref[did, pl.ds(first, DOC_CHUNK), :]
                table = (brows[:, None, :] * crows[None, :, :]).reshape(width, crows.shape[-1])
                acc += jnp.dot(
                    held[slot % 2, part, :, pl.ds(sub * width, width)],
                    table,
                    preferred_element_type=jnp.float32,
                )
        out_ref[qid] += acc
        return carry

    lax.fori_loop(0, used, step, 0)


def slot_terms(own_blocks, table, doc_blocks, ctx_blocks, n_q):
    slots, rows, width = own_blocks.shape
    rank = doc_blocks.shape[-1]
    pieces = 2
    cost = pl.CostEstimate(
        flops=2 * slots * rows * width * rank,
        bytes_accessed=own_blocks.size * 2 + n_q * rows * rank * 4,
        transcendentals=0,
    )
    return pl.pallas_call(
        slot_kernel,
        in_specs=[
            pl.BlockSpec(memory_space=pltpu.SMEM),
            pl.BlockSpec(memory_space=pl.ANY),
            pl.BlockSpec(memory_space=pltpu.VMEM),
            pl.BlockSpec(memory_space=pltpu.VMEM),
        ],
        out_specs=pl.BlockSpec(memory_space=pltpu.VMEM),
        out_shape=jax.ShapeDtypeStruct((n_q, rows, rank), jnp.float32),
        scratch_shapes=[
            pltpu.VMEM((2, pieces, rows, width // pieces), own_blocks.dtype),
            pltpu.SemaphoreType.DMA((2, pieces)),
        ],
        compiler_params=pltpu.CompilerParams(vmem_limit_bytes=VMEM_LIMIT),
        cost_estimate=cost,
    )(table, own_blocks, doc_blocks, ctx_blocks)


def slot_table(coords, counts):
    ids = coords[0, 0].T
    used = jnp.broadcast_to(counts[0].reshape(1, 1), (1, ids.shape[1]))
    return jnp.concatenate([ids, used], axis=0)


def body(blocks, coords, counts, doc_factor, ctx_factor):
    table = slot_table(coords, counts)
    table, ctx_factor = lax.optimization_barrier((table, ctx_factor))
    doc_slab = lax.all_gather(doc_factor, "row", axis=0, tiled=True)
    ctx_all = gather_rows(ctx_factor, "col")
    rank = doc_slab.shape[1]
    n_q = QBC * lax.axis_size("col")
    doc_blocks = doc_slab.reshape(-1, BD, rank)
    ctx_blocks = ctx_all.reshape(-1, BK, rank)
    parts = slot_terms(blocks[0, 0], table, doc_blocks, ctx_blocks, n_q)
    return lax.all_to_all(parts, "col", 0, 0, tiled=True).sum(axis=0)


def solution(mesh):
    placed = (
        P("row", "col", None, None, None),
        P("row", "col", None, None),
        P("row", "col"),
        P(("col", "row"), None),
        P("col", None),
    )
    return jax.shard_map(
        body, mesh=mesh, in_specs=placed, out_specs=P(("row", "col"), None), check_vma=False
    )
```

```python
import jax
import jax.numpy as jnp
from jax import lax
from jax.experimental import pallas as pl
from jax.experimental.pallas import tpu as pltpu
from jax.sharding import PartitionSpec as P

BQ = 128
BD = 128
BK = 64
QBC = 1
DOC_CHUNK = 32
VMEM_LIMIT = 50 * 1024 * 1024


def gather_rows(piece, axis):
    copies = jnp.broadcast_to(piece[None], (lax.axis_size(axis),) + piece.shape)
    gathered = lax.all_to_all(copies, axis, 0, 0, tiled=True)
    return gathered.reshape(-1, piece.shape[-1])


def slot_kernel(coords_ref, count_ref, blocks_hbm, doc_ref, ctx_ref, out_ref, held, sems):
    n_doc = doc_ref.shape[0]
    n_ctx = ctx_ref.shape[0]
    n_q = out_ref.shape[0]
    slots = blocks_hbm.shape[0]
    pieces = held.shape[1]
    piece = held.shape[-1]
    used = jnp.clip(count_ref[0], 0, slots)

    def fetch(slot, part):
        return pltpu.make_async_copy(
            blocks_hbm.at[slot, :, pl.ds(part * piece, piece)],
            held.at[slot % 2, part],
            sems.at[slot % 2, part],
        )

    @pl.when(used > 0)
    def _():
        for part in range(pieces):
            fetch(0, part).start()

    out_ref[...] = jnp.zeros_like(out_ref)

    def step(slot, carry):
        @pl.when(slot + 1 < used)
        def _():
            for part in range(pieces):
                fetch(slot + 1, part).start()

        qid = jnp.clip(coords_ref[0, slot], 0, n_q - 1)
        did = jnp.clip(coords_ref[1, slot], 0, n_doc - 1)
        kid = jnp.clip(coords_ref[2, slot], 0, n_ctx - 1)
        crows = ctx_ref[kid]
        width = DOC_CHUNK * BK
        acc = jnp.zeros(out_ref.shape[1:], jnp.float32)
        for part in range(pieces):
            fetch(slot, part).wait()
            for sub in range(piece // width):
                first = (part * piece + sub * width) // BK
                brows = doc_ref[did, pl.ds(first, DOC_CHUNK), :]
                table = (brows[:, None, :] * crows[None, :, :]).reshape(width, crows.shape[-1])
                acc += jnp.dot(
                    held[slot % 2, part, :, pl.ds(sub * width, width)],
                    table,
                    preferred_element_type=jnp.float32,
                )
        out_ref[qid] += acc
        return carry

    lax.fori_loop(0, used, step, 0)


def slot_terms(own_blocks, own_coords, used, doc_blocks, ctx_blocks, n_q):
    slots, rows, width = own_blocks.shape
    rank = doc_blocks.shape[-1]
    pieces = 2
    cost = pl.CostEstimate(
        flops=2 * slots * rows * width * rank,
        bytes_accessed=own_blocks.size * 2 + n_q * rows * rank * 4,
        transcendentals=0,
    )
    return pl.pallas_call(
        slot_kernel,
        in_specs=[
            pl.BlockSpec(memory_space=pltpu.SMEM),
            pl.BlockSpec(memory_space=pltpu.SMEM),
            pl.BlockSpec(memory_space=pl.ANY),
            pl.BlockSpec(memory_space=pltpu.VMEM),
            pl.BlockSpec(memory_space=pltpu.VMEM),
        ],
        out_specs=pl.BlockSpec(memory_space=pltpu.VMEM),
        out_shape=jax.ShapeDtypeStruct((n_q, rows, rank), jnp.float32),
        scratch_shapes=[
            pltpu.VMEM((2, pieces, rows, width // pieces), own_blocks.dtype),
            pltpu.SemaphoreType.DMA((2, pieces)),
        ],
        compiler_params=pltpu.CompilerParams(vmem_limit_bytes=VMEM_LIMIT),
        cost_estimate=cost,
    )(own_coords.T, used.reshape(-1), own_blocks, doc_blocks, ctx_blocks)


def body(blocks, coords, counts, doc_factor, ctx_factor):
    doc_slab = lax.all_gather(doc_factor, "row", axis=0, tiled=True)
    ctx_all = gather_rows(ctx_factor, "col")
    rank = doc_slab.shape[1]
    n_q = QBC * lax.axis_size("col")
    doc_blocks = doc_slab.reshape(-1, BD, rank)
    ctx_blocks = ctx_all.reshape(-1, BK, rank)
    parts = slot_terms(blocks[0, 0], coords[0, 0], counts[0], doc_blocks, ctx_blocks, n_q)
    return lax.all_to_all(parts, "col", 0, 0, tiled=True).sum(axis=0)


def solution(mesh):
    placed = (
        P("row", "col", None, None, None),
        P("row", "col", None, None),
        P("row", "col"),
        P(("col", "row"), None),
        P("col", None),
    )
    return jax.shard_map(
        body, mesh=mesh, in_specs=placed, out_specs=P(("row", "col"), None), check_vma=False
    )
```

```python
import jax
import jax.numpy as jnp
from jax import lax
from jax.experimental import pallas as pl
from jax.experimental.pallas import tpu as pltpu
from jax.sharding import PartitionSpec as P

BQ = 128
BD = 128
BK = 64
QBC = 1
DOC_CHUNK = 16
VMEM_LIMIT = 50 * 1024 * 1024


def gather_rows(piece, axis):
    copies = jnp.broadcast_to(piece[None], (lax.axis_size(axis),) + piece.shape)
    gathered = lax.all_to_all(copies, axis, 0, 0, tiled=True)
    return gathered.reshape(-1, piece.shape[-1])


def slot_kernel(coords_ref, count_ref, blocks_hbm, doc_ref, ctx_ref, out_ref, held, sems):
    n_doc = doc_ref.shape[0]
    n_ctx = ctx_ref.shape[0]
    n_q = out_ref.shape[0]
    slots = blocks_hbm.shape[0]
    total = held.shape[-1]
    cuts = (0, total // 4, total)
    pieces = len(cuts) - 1
    used = jnp.clip(count_ref[0], 0, slots)

    def fetch(slot, part):
        span = pl.ds(cuts[part], cuts[part + 1] - cuts[part])
        return pltpu.make_async_copy(
            blocks_hbm.at[slot, :, span],
            held.at[slot % 2, :, span],
            sems.at[slot % 2, part],
        )

    @pl.when(used > 0)
    def _():
        for part in range(pieces):
            fetch(0, part).start()

    out_ref[...] = jnp.zeros_like(out_ref)

    def step(slot, carry):
        @pl.when(slot + 1 < used)
        def _():
            for part in range(pieces):
                fetch(slot + 1, part).start()

        qid = jnp.clip(coords_ref[0, slot], 0, n_q - 1)
        did = jnp.clip(coords_ref[1, slot], 0, n_doc - 1)
        kid = jnp.clip(coords_ref[2, slot], 0, n_ctx - 1)
        crows = ctx_ref[kid]
        width = DOC_CHUNK * BK
        acc = jnp.zeros(out_ref.shape[1:], jnp.float32)
        for part in range(pieces):
            fetch(slot, part).wait()
            for column in range(cuts[part], cuts[part + 1], width):
                brows = doc_ref[did, pl.ds(column // BK, DOC_CHUNK), :]
                table = (brows[:, None, :] * crows[None, :, :]).reshape(width, crows.shape[-1])
                acc += jnp.dot(
                    held[slot % 2, :, pl.ds(column, width)],
                    table,
                    preferred_element_type=jnp.float32,
                )
        out_ref[qid] += acc
        return carry

    lax.fori_loop(0, used, step, 0)


def slot_terms(own_blocks, own_coords, used, doc_blocks, ctx_blocks, n_q):
    slots, rows, width = own_blocks.shape
    rank = doc_blocks.shape[-1]
    cost = pl.CostEstimate(
        flops=2 * slots * rows * width * rank,
        bytes_accessed=own_blocks.size * 2 + n_q * rows * rank * 4,
        transcendentals=0,
    )
    return pl.pallas_call(
        slot_kernel,
        in_specs=[
            pl.BlockSpec(memory_space=pltpu.SMEM),
            pl.BlockSpec(memory_space=pltpu.SMEM),
            pl.BlockSpec(memory_space=pl.ANY),
            pl.BlockSpec(memory_space=pltpu.VMEM),
            pl.BlockSpec(memory_space=pltpu.VMEM),
        ],
        out_specs=pl.BlockSpec(memory_space=pltpu.VMEM),
        out_shape=jax.ShapeDtypeStruct((n_q, rows, rank), jnp.float32),
        scratch_shapes=[
            pltpu.VMEM((2, rows, width), own_blocks.dtype),
            pltpu.SemaphoreType.DMA((2, 2)),
        ],
        compiler_params=pltpu.CompilerParams(vmem_limit_bytes=VMEM_LIMIT),
        cost_estimate=cost,
    )(own_coords.T, used.reshape(-1), own_blocks, doc_blocks, ctx_blocks)


def body(blocks, coords, counts, doc_factor, ctx_factor):
    doc_slab = lax.all_gather(doc_factor, "row", axis=0, tiled=True)
    ctx_all = gather_rows(ctx_factor, "col")
    rank = doc_slab.shape[1]
    n_q = QBC * lax.axis_size("col")
    doc_blocks = doc_slab.reshape(-1, BD, rank)
    ctx_blocks = ctx_all.reshape(-1, BK, rank)
    parts = slot_terms(blocks[0, 0], coords[0, 0], counts[0], doc_blocks, ctx_blocks, n_q)
    return lax.all_to_all(parts, "col", 0, 0, tiled=True).sum(axis=0)


def solution(mesh):
    placed = (
        P("row", "col", None, None, None),
        P("row", "col", None, None),
        P("row", "col"),
        P(("col", "row"), None),
        P("col", None),
    )
    return jax.shard_map(
        body, mesh=mesh, in_specs=placed, out_specs=P(("row", "col"), None), check_vma=False
    )
```
